256 devices in a mesh: tm: 64 (over y_lo, z, x), prod: 4 (over y_hi, core).
Axes of the slice: x: 4, y: 4 (y_hi: 2, y_lo: 2; y = y_hi * 2 + y_lo), z: 8, core: 2. Of those that a mesh axis runs over, the one named last changes fastest.
Arguments:
- sales_records: float32 [2048, 64, 16, 128], P('tm', 'prod'), may hold values from -6 to 6
- day_month: int32 [2048], replicated, may hold values from 0 to 63, as said below
- month_year: int32 [64], replicated, may hold values from 0 to 7, never falling along the last dimension, each value on 1 to 16 neighbouring positions
- product_category: int32 [64], replicated, may hold values from 0 to 31
- store_region: int32 [16], replicated, may hold values from 0 to 3
Outputs:
- month_detail: float32 [64, 32, 4, 128], P('tm', 'prod')
- month_category: float32 [64, 32, 128], P('tm', 'prod')
- month_region: float32 [64, 4, 128], P('tm')
- month_totals: float32 [64, 128], P('tm')
- year_detail: float32 [8, 32, 4, 128], replicated
- year_category: float32 [8, 32, 128], replicated
- year_region: float32 [8, 4, 128], replicated
- year_totals: float32 [8, 128], replicated
The draws below stay inside these ranges and needn't reach their ends.
Inputs may be any that keep to these rules, and one draw needn't show every extreme that they name: `day_month`: never falls along the days; month m, for m of 1 to 63, begins at a day from m * 32 - 31 // 2 to m * 32 + 31 // 2, and both ends of that range are taken in every draw. `month_year`: never falls along the months; every year has 1 to 16 months, one exactly that many.
All inputs are finite; a program needn't handle non-finite values.
Results may differ from the reference program's by a relative error of at most 0.0001.
Values sent between devices are 32-bit elements; how exact they have to be, the bound alone decides.
A program may use at most 64 MiB of HBM per device.

```python
import math
import jax
import jax.numpy as jnp
import numpy as np
from jax import lax

DAYS_PER_INDEX = 32
STORE_COUNT = 16
MEASURE_COUNT = 128
CATEGORY_COUNT = 32
REGION_COUNT = 4
TOTAL_DAYS = 2048
PRODUCT_COUNT = 64
TOTAL_MONTHS = 64
YEARS = 8
N_TM = 64


def draw_day_month(key, part):
    half = (DAYS_PER_INDEX - 1) // 2
    inner = TOTAL_MONTHS - 1
    jitter = jax.random.randint(jax.random.fold_in(key, 11), (inner,), -half, half + 1)
    places = jnp.arange(inner, dtype=jnp.int32)
    middle = TOTAL_MONTHS // 2
    jitter = jnp.where(places == 0, -half, jitter)
    jitter = jnp.where(places == middle - 2, -half, jitter)
    jitter = jnp.where(places == middle - 1, half, jitter)
    jitter = jnp.where(places == middle, half, jitter)
    bounds = (places + 1) * DAYS_PER_INDEX + jitter
    days = jnp.arange(TOTAL_DAYS, dtype=jnp.int32)
    return jnp.sum((days[:, None] >= bounds[None, :]).astype(jnp.int32), 1).astype(jnp.int32)


def with_ends(result, rng, low, high):
    dims = result.shape
    place = [jax.random.randint(jax.random.fold_in(rng, axis), (), 0, dims[axis]) for axis in range(len(dims))]
    result = result.at[tuple(place)].set(low)
    longest = dims.index(max(dims))
    place[longest] = (place[longest] + 1) % dims[longest]
    return result.at[tuple(place)].set(high)


def shard_levels(own_key, extent, split, smallest, top_value):
    def one(position, parts):
        draws = jax.random.uniform(jax.random.fold_in(jax.random.fold_in(own_key, 6), position), (parts,), jnp.float32, smallest / len(split), top_value / len(split))
        return jnp.repeat(jnp.exp(draws), extent[position] // parts).reshape((-1,) + (1,) * (len(extent) - position - 1))

    factor_of = one(*split[0])
    for cut in split[1:]:
        factor_of = factor_of * one(*cut)
    return factor_of


def length_profile(number_of, total, bound, slope):
    loads = [(1 << 20) // math.isqrt(grade ** slope) + 1 for grade in range(2, number_of + 1)]
    spare, given = total - bound - (number_of - 1), [1] * (number_of - 1)
    while spare > 0:
        movable = [i for i in range(number_of - 1) if given[i] < bound]
        pool, left = sum([loads[i] for i in movable]), spare
        for i in movable:
            addition = min(bound - given[i], max(1, left * loads[i] // pool), spare)
            given[i] = given[i] + addition
            spare = spare - addition
    return np.array([bound] + given)


def ragged_sizes(rng, amount, total, reach, slope):
    if amount == 2:
        one = jax.random.randint(rng, (), max(1, total - reach), min(reach, total - 1) + 1)
        return jnp.stack([one, total - one])
    sizes = jnp.asarray(length_profile(amount, total, reach, slope), jnp.int32)
    pairs = (amount - 1) // 2
    donor, sink = sizes[1:1 + 2 * pairs:2], sizes[2:2 + 2 * pairs:2]
    margin = jnp.minimum(donor - 1, reach - sink)
    passed = jax.random.randint(jax.random.fold_in(rng, 1), (pairs,), 0, 1 << 20) % (margin + 1)
    sizes = sizes.at[1:1 + 2 * pairs:2].set(donor - passed).at[2:2 + 2 * pairs:2].set(sink + passed)
    return sizes[jax.random.permutation(jax.random.fold_in(rng, 2), amount)]


def bell_draw(own_key, dims, deviation, limit, shards=(), held_as=jnp.bfloat16):
    entries = deviation * jax.random.normal(own_key, dims, jnp.float32)
    if shards:
        entries = entries * shard_levels(own_key, dims, shards, -0.22, 0.18)
    return jnp.clip(entries, -limit, limit).astype(held_as)


def setup_inputs(seed: int = 0) -> dict:
    keys = jax.random.split(jax.random.key(seed), 6)
    sales_records = bell_draw(keys[0], (TOTAL_DAYS, PRODUCT_COUNT, STORE_COUNT, MEASURE_COUNT), 1.0, 6.0, ((0, 64), (1, 4)), jnp.float32)
    day_month = draw_day_month(jax.random.fold_in(keys[5], 71), 0)
    month_year = jnp.searchsorted(jnp.cumsum(ragged_sizes(keys[2], YEARS, TOTAL_MONTHS, 2 * TOTAL_MONTHS // YEARS, 1)), jnp.arange(TOTAL_MONTHS), side="right").astype(jnp.int32)
    product_category = with_ends(jax.random.randint(keys[3], (PRODUCT_COUNT,), 0, CATEGORY_COUNT), jax.random.fold_in(keys[3], 1), 0, CATEGORY_COUNT - 1).astype(jnp.int32)
    store_region = with_ends(jax.random.randint(keys[4], (STORE_COUNT,), 0, REGION_COUNT), jax.random.fold_in(keys[4], 1), 0, REGION_COUNT - 1).astype(jnp.int32)
    return dict(sales_records=sales_records, day_month=day_month, month_year=month_year, product_category=product_category, store_region=store_region)


def onehot(labels, width):
    return (labels[:, None] == jnp.arange(width, dtype=jnp.int32)[None, :]).astype(jnp.float32)

def scaled(sums, counts):
    return sums / jnp.sqrt(counts)

def reference(sales_records, day_month, month_year, product_category, store_region):
    highest = lax.Precision.HIGHEST
    month_hot = onehot(day_month, TOTAL_MONTHS)
    year_hot = onehot(month_year, YEARS)
    category_hot = onehot(product_category, CATEGORY_COUNT)
    region_hot = onehot(store_region, REGION_COUNT)
    daily_blocks = sales_records.reshape(N_TM, DAYS_PER_INDEX, PRODUCT_COUNT, STORE_COUNT, MEASURE_COUNT)
    month_blocks = month_hot.reshape(N_TM, DAYS_PER_INDEX, TOTAL_MONTHS)

    def accumulate(running, pieces):
        day_block, block_hot = pieces
        by_region = jnp.einsum('dpsq,sr->dprq', day_block, region_hot, precision=highest)
        by_category = jnp.einsum('dprq,pc->dcrq', by_region, category_hot, precision=highest)
        return (running + jnp.einsum('dcrq,dm->mcrq', by_category, block_hot, precision=highest), None)
    start_offset = jnp.zeros((TOTAL_MONTHS, CATEGORY_COUNT, REGION_COUNT, MEASURE_COUNT), jnp.float32)
    cube, _ = lax.scan(accumulate, start_offset, (daily_blocks, month_blocks))
    year_cube = jnp.einsum('mcrq,my->ycrq', cube, year_hot, precision=highest)
    month_days = lax.optimization_barrier(jnp.sum(month_hot, 0))
    year_days = jnp.dot(month_days, year_hot, precision=highest)
    category_size = lax.optimization_barrier(jnp.sum(category_hot, 0))
    region_size = lax.optimization_barrier(jnp.sum(region_hot, 0))
    stores = float(STORE_COUNT)
    products = float(PRODUCT_COUNT)

    def four_nodes(detail, period_days):
        cell = period_days[:, None, None] * category_size[None, :, None] * region_size[None, None, :]
        first = scaled(detail, jnp.maximum(cell, 1.0)[..., None])
        by_cat = lax.optimization_barrier(jnp.sum(detail, 2))
        second = scaled(by_cat, jnp.maximum(period_days[:, None] * category_size[None, :] * stores, 1.0)[..., None])
        by_reg = lax.optimization_barrier(jnp.sum(detail, 1))
        third = scaled(by_reg, jnp.maximum(period_days[:, None] * products * region_size[None, :], 1.0)[..., None])
        fourth = scaled(lax.optimization_barrier(jnp.sum(by_reg, 1)), (period_days * products * stores)[:, None])
        return (first, second, third, fourth)
    month_detail, month_category, month_region, month_totals = four_nodes(cube, month_days)
    year_detail, year_category, year_region, year_totals = four_nodes(year_cube, year_days)
    return (month_detail, month_category, month_region, month_totals, year_detail, year_category, year_region, year_totals)
```

```python
import jax
import jax.numpy as jnp
from jax import lax
from jax.experimental import pallas as pl
from jax.experimental.pallas import tpu as pltpu
from jax.sharding import PartitionSpec as P

MESH = pl.DeviceIdType.MESH
F32 = jnp.float32
BF16 = jnp.bfloat16
I32 = jnp.int32

NX, NY, NZ = 4, 4, 8
TM, PROD = 64, 4
DAYS = 32
CHUNKS = 8
CHUNK_ROWS = 256 // CHUNKS


def hops(a, b):
    return min(a, 4 - a) + min(b, 4 - b)


PLANE = sorted(
    ((a, b, c) for a in range(4) for b in range(4) for c in range(2) if (a, b, c) != (0, 0, 0)),
    key=lambda o: -hops(o[0], o[1]),
)
CHIPS = sorted(
    ((a, b) for a in range(4) for b in range(4) if (a, b) != (0, 0)),
    key=lambda o: -hops(o[0], o[1]),
)
ZOFF = [4, 3, 5, 2, 6, 1, 7]
MONTH = [(k, p) for k in (0, 2, 1) for p in (2, 1, 3, 0) if (k, p) != (1, 0)]


def iota(shape, dim):
    return lax.broadcasted_iota(I32, shape, dim)


def split3(value):
    high = value.astype(BF16)
    rest = value - high.astype(F32)
    mid = rest.astype(BF16)
    low = (rest - mid.astype(F32)).astype(BF16)
    return high, mid, low


def inv_root(count):
    return 1.0 / jnp.sqrt(count)


def kernel(
    sales, day_month, month_year, product_category, store_region,
    year_detail, year_category, year_region, year_totals,
    month_detail, month_category, month_region, month_totals,
    days_v, years_v, cats_v, regs_v, days_s, years_s, cats_s, regs_s,
    x, y, part, pieces, plane_in, year_part, z_in, year_own, cube,
    month_in, month_sum, reg_out, reg_in, scale, sums_v, days_of,
    small_sem, load_sem, plane_ss, plane_rs, month_ss, month_rs, z_ss, z_rs,
    reg_ss, reg_rs, ag_ss, ag_rs, core_ss, core_rs,
):
    t, prod = lax.axis_index("tm"), lax.axis_index("prod")
    px, pz, ylo = t % NX, (t // NX) % NZ, t // (NX * NZ)
    core, yhi = prod % 2, prod // 2
    py = yhi * 2 + ylo

    def at(ax, ay, az, ac):
        return (ay % 2) * (NX * NZ) + az * NX + ax, (ay // 2) * 2 + ac

    def category_of(ax, ay, ac):
        return ((ay // 2) * 2 + ac) * 8 + (ay % 2) * NX + ax

    own_cat = category_of(px, py, core)
    sibling = (t, prod + 1 - 2 * core)

    barrier = pltpu.get_barrier_semaphore()

    def greet(who):
        pl.semaphore_signal(barrier, inc=1, device_id=who, device_id_type=MESH)

    def plane_peer(o):
        return at((px + o[0]) % NX, (py + o[1]) % NY, pz, (core + o[2]) % 2)

    def z_peer(d):
        return at(px, py, (pz + d) % NZ, core)

    for d in ZOFF:
        greet(z_peer(d))
    for o in PLANE:
        greet(plane_peer(o))
    for p in range(PROD):
        greet(((t + 1) % TM, p))
        greet(((t + TM - 1) % TM, p))

    loads = [
        pltpu.make_async_copy(
            sales.at[:, pl.ds(i * CHUNK_ROWS, CHUNK_ROWS), :],
            x.at[:, pl.ds(i * CHUNK_ROWS, CHUNK_ROWS), :],
            load_sem.at[i],
        )
        for i in range(CHUNKS)
    ]
    smalls = [
        pltpu.make_async_copy(a, b, small_sem.at[i])
        for i, (a, b) in enumerate((
            (day_month, days_s), (product_category, cats_s), (store_region, regs_s),
            (month_year, years_s), (day_month, days_v), (product_category, cats_v),
            (store_region, regs_v), (month_year, years_v),
        ))
    ]
    for copy in smalls[:3]:
        copy.start()
    for copy in loads:
        copy.start()
    for copy in smalls[3:]:
        copy.start()
    for copy in smalls:
        copy.wait()

    lane = iota((8, 256), 1)
    key = jnp.zeros((8, 256), I32)
    for p in range(16):
        key = jnp.where(lane // 16 == p, cats_s[0, prod * 16 + p] * 4, key)
    reg = jnp.zeros((8, 256), I32)
    for s in range(16):
        reg = jnp.where(lane % 16 == s, regs_s[0, s], reg)
    key = key + reg
    hot = jnp.concatenate(
        [jnp.where(iota((8, 256), 0) + 8 * i == key, 1.0, 0.0) for i in range(16)], axis=0
    ).astype(BF16)

    row0 = t // 4
    lane0 = (t % 4) * DAYS
    masks = []
    for d in range(DAYS):
        month = days_s[row0, lane0 + d]
        other = t - 1 if d < DAYS // 2 else t + 1
        masks.append(jnp.full((8, 128), jnp.where(month == other, 1.0, 0.0), F32))

    def reduce_rows(i, carry):
        rows = pl.ds(pl.multiple_of(i * 8, 8), 8)
        mid = [jnp.zeros((8, 128), F32) for _ in range(2)]
        side = []
        for half in range(2):
            acc = jnp.zeros((8, 128), F32)
            for d in range(half * 16, half * 16 + 16):
                value = x[d, rows, :]
                kept = value * masks[d]
                acc = acc + kept
                mid[half] = mid[half] + (value - kept)
            side.append(acc)
        y[rows, 0:128] = side[0]
        y[rows, 128:256] = mid[0] + mid[1]
        y[rows, 256:384] = side[1]
        return carry

    for c in range(CHUNKS):
        loads[c].wait()
        lax.fori_loop(c * CHUNK_ROWS // 8, (c + 1) * CHUNK_ROWS // 8, reduce_rows, 0)

    def hot_sum(value):
        return sum(
            jnp.dot(hot, piece, preferred_element_type=F32) for piece in split3(value)
        )

    low = iota((8, 128), 0) < 4
    slots = [hot_sum(y[:, 128 * k : 128 * k + 128]) for k in range(3)]
    for k in range(3):
        part[k] = slots[k]
    for i in range(16):
        a, b, c = (slots[k][8 * i : 8 * i + 8] for k in range(3))
        pieces[2 * i, 0:8] = jnp.where(low, a, pltpu.roll(b, 4, 0))
        pieces[2 * i, 8:16] = c
        pieces[2 * i + 1, 0:8] = jnp.where(low, pltpu.roll(a, 4, 0), b)
        pieces[2 * i + 1, 8:16] = pltpu.roll(c, 4, 0)

    pl.semaphore_wait(barrier, len(ZOFF) + len(PLANE) + 2 * PROD)

    plane_copies = []
    for k, o in enumerate(PLANE):
        ax, ay, ac = (px + o[0]) % NX, (py + o[1]) % NY, (core + o[2]) % 2
        plane_copies.append(pltpu.make_async_remote_copy(
            src_ref=pieces.at[category_of(ax, ay, ac), pl.ds(0, 12), :],
            dst_ref=plane_in.at[k, pl.ds(0, 12), :],
            send_sem=plane_ss.at[k], recv_sem=plane_rs.at[k],
            device_id=at(ax, ay, pz, ac), device_id_type=MESH,
        ))
    for copy in plane_copies:
        copy.start()
    month_copies = []
    for n, (k, p) in enumerate(MONTH):
        to = (prod + p) % PROD
        month_copies.append(pltpu.make_async_remote_copy(
            src_ref=part.at[k, pl.ds(pl.multiple_of(to * 32, 32), 32), :],
            dst_ref=month_in.at[n],
            send_sem=month_ss.at[n], recv_sem=month_rs.at[n],
            device_id=((t + k - 1 + TM) % TM, to), device_id_type=MESH,
        ))
    for copy in month_copies:
        copy.start()

    months = iota((64, 128), 0)
    found = jnp.zeros((64, 128), F32)
    own_found = jnp.zeros((8, 128), F32)
    for i in range(16):
        line = days_v[i : i + 1, :]
        found = found + jnp.where(months == line, 1.0, 0.0)
    month_days = jnp.broadcast_to(jnp.sum(found, axis=1, keepdims=True), (64, 128))
    for i in range(2):
        own_found = own_found + jnp.where(days_v[8 * i : 8 * i + 8, :] == t, 1.0, 0.0)
    own_days = jnp.broadcast_to(
        jnp.sum(jnp.sum(own_found, axis=1, keepdims=True), axis=0, keepdims=True), (8, 128)
    )
    row32, lane64 = iota((32, 64), 0), iota((8, 64), 0)
    years_of = jnp.where(row32 // 4 == years_v[0:1, :], 1.0, 0.0).astype(BF16)
    year_days = jnp.dot(years_of, month_days.astype(BF16), preferred_element_type=F32)
    cats_of = cats_v[0:1, :]
    sizes = jnp.broadcast_to(
        jnp.sum(jnp.where(row32 == cats_of, 1.0, 0.0), axis=1, keepdims=True), (32, 128)
    )
    own_sizes = jnp.broadcast_to(
        jnp.sum(jnp.where(row32 // 4 + prod * 8 == cats_of, 1.0, 0.0), axis=1, keepdims=True),
        (32, 128),
    )
    own_sizes8 = jnp.broadcast_to(
        jnp.sum(jnp.where(lane64 + prod * 8 == cats_of, 1.0, 0.0), axis=1, keepdims=True),
        (8, 128),
    )
    regions = jnp.broadcast_to(
        jnp.sum(jnp.where(iota((32, 16), 0) % 4 == regs_v[0:1, :], 1.0, 0.0), axis=1, keepdims=True),
        (32, 128),
    )
    regions8 = regions[0:8]
    year_region_days = year_days * regions

    target = [jnp.where(low, 2 * i, 2 * i + 1) for i in range(4)]
    totals = [jnp.zeros((8, 128), F32) for _ in range(4)]

    def year_of(time, k):
        return years_s[0, jnp.clip(time + k - 1, 0, TM - 1)]

    gathered = {}
    for k, o in enumerate(PLANE):
        gathered.setdefault((o[0], o[1] % 2), []).append(k)
    for (dx, dy), ks in sorted(gathered.items(), key=lambda g: max(hops(*PLANE[k][:2]) for k in g[1])):
        if (dx, dy) == (0, 0):
            first, second = pieces[own_cat, 0:8], pieces[own_cat, 8:16]
        else:
            first = second = None
        for k in ks:
            plane_copies[k].wait_recv()
            one, two = plane_in[k, 0:8], plane_in[k, 8:16]
            first = one if first is None else first + one
            second = two if second is None else second + two
        time = ((py - dy + NY) % 2) * (NX * NZ) + pz * NX + (px - dx + NX) % NX
        year0, year1, year2 = (year_of(time, k) for k in range(3))
        swapped = pltpu.roll(first, 4, 0)
        second = jnp.where(low, second, pltpu.roll(second, 4, 0))
        straight_of = jnp.where(low, year0, year1)
        swapped_of = jnp.where(low, year1, year0)
        second_of = jnp.where(low, year2, year2)
        for i in range(4):
            totals[i] = totals[i] + (
                jnp.where(straight_of == target[i], first, 0.0)
                + jnp.where(swapped_of == target[i], swapped, 0.0)
                + jnp.where(second_of == target[i], second, 0.0)
            )
    for i in range(4):
        year_part[8 * i : 8 * i + 8, :] = totals[i]
    z_copies = [
        pltpu.make_async_remote_copy(
            src_ref=year_part, dst_ref=z_in.at[k], send_sem=z_ss.at[k], recv_sem=z_rs.at[k],
            device_id=z_peer(d), device_id_type=MESH,
        )
        for k, d in enumerate(ZOFF)
    ]
    for copy in z_copies:
        copy.start()

    month = part[1, pl.ds(pl.multiple_of(prod * 32, 32), 32), :]
    for n, copy in enumerate(month_copies):
        copy.wait_recv()
        month = month + month_in[n]
    month_sum[...] = month
    own_reg = month[0:8] + month[8:16] + month[16:24] + month[24:32]
    own_reg = own_reg + pltpu.roll(own_reg, 4, 0)
    reg_out[...] = own_reg
    reg_copies = [
        pltpu.make_async_remote_copy(
            src_ref=reg_out, dst_ref=reg_in.at[p - 1],
            send_sem=reg_ss.at[p - 1], recv_sem=reg_rs.at[p - 1],
            device_id=(t, (prod + p) % PROD), device_id_type=MESH,
        )
        for p in range(1, PROD)
    ]
    for copy in reg_copies:
        copy.start()
    days32 = jnp.concatenate([own_days] * 4, axis=0)
    month_detail[...] = month * inv_root(jnp.maximum(days32 * own_sizes * regions, 1.0))
    by_cat = sum(month_sum[pl.ds(r, 8, stride=4), :] for r in range(4))
    month_category[...] = by_cat * inv_root(jnp.maximum(own_days * own_sizes8 * 16.0, 1.0))

    for c in range(32):
        scale[32 * c : 32 * c + 32, :] = inv_root(
            jnp.maximum(year_region_days * jnp.broadcast_to(sizes[c : c + 1, :], (32, 128)), 1.0)
        )

    year = year_part[...]
    for k, copy in reversed(list(enumerate(z_copies))):
        copy.wait_recv()
        year = year + z_in[k]
    year_own[...] = year
    own_rows = cube.at[pl.ds(pl.multiple_of(own_cat * 32, 32), 32), :]
    ag_copies = []
    for k, (dx, dy) in enumerate(CHIPS):
        ag_copies.append(pltpu.make_async_remote_copy(
            src_ref=year_own, dst_ref=own_rows, send_sem=ag_ss.at[k], recv_sem=ag_rs.at[k],
            device_id=at((px + dx) % NX, (py + dy) % NY, pz, core), device_id_type=MESH,
        ))
    for copy in ag_copies:
        copy.start()
    core_copies = [pltpu.make_async_remote_copy(
        src_ref=year_own, dst_ref=own_rows, send_sem=core_ss.at[15], recv_sem=core_rs.at[15],
        device_id=sibling, device_id_type=MESH,
    )]
    core_copies[0].start()
    cube[pl.ds(pl.multiple_of(own_cat * 32, 32), 32), :] = year

    region = own_reg
    for p, copy in enumerate(reg_copies):
        copy.wait_recv()
        region = region + reg_in[p]
    month_region[...] = region * inv_root(jnp.maximum(own_days * 64.0 * regions8, 1.0))
    total = jnp.sum(jnp.where(low, region, 0.0), axis=0, keepdims=True)
    month_totals[...] = jnp.broadcast_to(total, (8, 128)) * inv_root(own_days * 64.0 * 16.0)

    for k in reversed(range(len(CHIPS))):
        dx, dy = CHIPS[k]
        ag_copies[k].wait_recv()
        cat = category_of((px - dx + NX) % NX, (py - dy + NY) % NY, core)
        rows = cube.at[pl.ds(pl.multiple_of(cat * 32, 32), 32), :]
        copy = pltpu.make_async_remote_copy(
            src_ref=rows, dst_ref=rows, send_sem=core_ss.at[k], recv_sem=core_rs.at[k],
            device_id=sibling, device_id_type=MESH,
        )
        copy.start()
        core_copies.append(copy)
    for copy in core_copies:
        copy.wait_recv()

    sums = jnp.zeros((32, 128), F32)
    for i in range(16):
        a = cube[64 * i : 64 * i + 32, :]
        b = cube[64 * i + 32 : 64 * i + 64, :]
        sums = sums + (a + b)
        a = a * scale[64 * i : 64 * i + 32, :]
        b = b * scale[64 * i + 32 : 64 * i + 64, :]
        for n in range(4):
            one, two = a[8 * n : 8 * n + 8], b[8 * n : 8 * n + 8]
            year_detail[(2 * n) * 128 + 8 * i : (2 * n) * 128 + 8 * i + 8, :] = jnp.where(
                low, one, pltpu.roll(two, 4, 0))
            year_detail[(2 * n + 1) * 128 + 8 * i : (2 * n + 1) * 128 + 8 * i + 8, :] = jnp.where(
                low, pltpu.roll(one, 4, 0), two)
    sums_v[...] = sums
    year_region[...] = sums * inv_root(jnp.maximum(year_region_days * 64.0, 1.0))
    for n in range(8):
        by_cat = sum(cube[pl.ds(4 * n + r, 32, stride=32), :] for r in range(4))
        days = jnp.broadcast_to(year_days[4 * n : 4 * n + 1, :], (32, 128))
        year_category[32 * n : 32 * n + 32, :] = by_cat * inv_root(
            jnp.maximum(days * sizes * 16.0, 1.0))
    days_of[...] = year_days
    days8 = days_of[pl.ds(0, 8, stride=4), :]
    total = sum(sums_v[pl.ds(r, 8, stride=4), :] for r in range(4))
    year_totals[...] = total * inv_root(days8 * 64.0 * 16.0)

    for copy in plane_copies + month_copies + z_copies + reg_copies + ag_copies + core_copies:
        copy.wait_send()


def finish(*refs):
    half = len(refs) // 2
    for source, target in zip(refs[:half], refs[half:]):
        target[...] = source[0 : target.shape[0], :]


def shape(rows):
    return jax.ShapeDtypeStruct((rows, 128), F32)


def shards(sales_records, day_month, month_year, product_category, store_region):
    vmem = pl.BlockSpec(memory_space=pltpu.VMEM)
    anywhere = pl.BlockSpec(memory_space=pl.ANY)
    dma = pltpu.SemaphoreType.DMA
    found = pl.pallas_call(
        kernel,
        out_shape=[shape(n) for n in (1024, 256, 32, 8, 32, 8, 8, 8)],
        in_specs=[anywhere] * 5,
        out_specs=[vmem] * 8,
        scratch_shapes=[
            pltpu.VMEM((16, 128), I32), pltpu.VMEM((1, 64), I32),
            pltpu.VMEM((1, 64), I32), pltpu.VMEM((1, 16), I32),
            pltpu.SMEM((16, 128), I32), pltpu.SMEM((1, 64), I32),
            pltpu.SMEM((1, 64), I32), pltpu.SMEM((1, 16), I32),
            pltpu.VMEM((32, 256, 128), F32),
            pltpu.VMEM((256, 384), F32),
            pltpu.VMEM((3, 128, 128), F32),
            pltpu.VMEM((32, 16, 128), F32),
            pltpu.VMEM((31, 16, 128), F32),
            pltpu.VMEM((32, 128), F32),
            pltpu.VMEM((7, 32, 128), F32),
            pltpu.VMEM((32, 128), F32),
            pltpu.VMEM((1024, 128), F32),
            pltpu.VMEM((11, 32, 128), F32),
            pltpu.VMEM((32, 128), F32),
            pltpu.VMEM((8, 128), F32),
            pltpu.VMEM((3, 8, 128), F32),
            pltpu.VMEM((1024, 128), F32),
            pltpu.VMEM((32, 128), F32),
            pltpu.VMEM((32, 128), F32),
            dma((8,)), dma((CHUNKS,)), dma((31,)), dma((31,)), dma((11,)), dma((11,)),
            dma((7,)), dma((7,)), dma((3,)), dma((3,)), dma((15,)), dma((15,)),
            dma((16,)), dma((16,)),
        ],
        compiler_params=pltpu.CompilerParams(collective_id=0, has_side_effects=True),
        name="cube",
    )(
        sales_records.reshape(32, 256, 128),
        day_month.reshape(16, 128),
        month_year.reshape(1, 64),
        product_category.reshape(1, 64),
        store_region.reshape(1, 16),
    )
    out = pl.pallas_call(
        finish,
        out_shape=[shape(n) for n in (1024, 256, 32, 8, 32, 8, 4, 1)],
        in_specs=[vmem] * 8,
        out_specs=[vmem] * 8,
        name="finish",
    )(*found)
    yd, yc, yr, yt, md, mc, mr, mt = out
    return (
        md.reshape(1, 8, 4, 128), mc.reshape(1, 8, 128), mr.reshape(1, 4, 128), mt.reshape(1, 128),
        yd.reshape(8, 32, 4, 128), yc.reshape(8, 32, 128), yr.reshape(8, 4, 128), yt,
    )


def solution(mesh):
    placed = (P("tm", "prod", None, None), P(), P(), P(), P())
    return jax.shard_map(
        shards,
        mesh=mesh,
        in_specs=placed,
        out_specs=(
            P("tm", "prod", None, None), P("tm", "prod", None), P("tm", None, None), P("tm", None),
            P(), P(), P(), P(),
        ),
        check_vma=False,
    )
```

```python
import jax
import jax.numpy as jnp
from jax import lax
from jax.experimental import pallas as pl
from jax.experimental.pallas import tpu as pltpu
from jax.sharding import PartitionSpec as P

MESH = pl.DeviceIdType.MESH
F32 = jnp.float32
BF16 = jnp.bfloat16
I32 = jnp.int32

NX, NY, NZ = 4, 4, 8
TM, PROD = 64, 4
DAYS = 32
CHUNKS = 8
CHUNK_ROWS = 256 // CHUNKS


def hops(a, b):
    return min(a, 4 - a) + min(b, 4 - b)


PLANE = sorted(
    ((a, b, c) for a in range(4) for b in range(4) for c in range(2) if (a, b, c) != (0, 0, 0)),
    key=lambda o: -hops(o[0], o[1]),
)
CHIPS = sorted(
    ((a, b) for a in range(4) for b in range(4) if (a, b) != (0, 0)),
    key=lambda o: -hops(o[0], o[1]),
)
ZOFF = [4, 3, 5, 2, 6, 1, 7]
MONTH = [(k, p) for k in (0, 2, 1) for p in (2, 1, 3, 0) if (k, p) != (1, 0)]


def iota(shape, dim):
    return lax.broadcasted_iota(I32, shape, dim)


def split3(value):
    high = value.astype(BF16)
    rest = value - high.astype(F32)
    mid = rest.astype(BF16)
    low = (rest - mid.astype(F32)).astype(BF16)
    return high, mid, low


def inv_root(count):
    return 1.0 / jnp.sqrt(count)


def kernel(
    sales, day_month, month_year, product_category, store_region,
    year_detail, year_category, year_region, year_totals,
    month_detail, month_category, month_region, month_totals,
    days_v, years_v, cats_v, regs_v, days_s, years_s, cats_s, regs_s,
    x, y, part, pieces, plane_in, year_part, z_in, year_own, cube,
    month_in, month_sum, reg_out, reg_in, scale, sums_v, days_of,
    small_sem, load_sem, plane_ss, plane_rs, month_ss, month_rs, z_ss, z_rs,
    reg_ss, reg_rs, ag_ss, ag_rs, core_ss, core_rs,
):
    t, prod = lax.axis_index("tm"), lax.axis_index("prod")
    px, pz, ylo = t % NX, (t // NX) % NZ, t // (NX * NZ)
    core, yhi = prod % 2, prod // 2
    py = yhi * 2 + ylo

    def at(ax, ay, az, ac):
        return (ay % 2) * (NX * NZ) + az * NX + ax, (ay // 2) * 2 + ac

    def category_of(ax, ay, ac):
        return ((ay // 2) * 2 + ac) * 8 + (ay % 2) * NX + ax

    own_cat = category_of(px, py, core)
    sibling = (t, prod + 1 - 2 * core)

    barrier = pltpu.get_barrier_semaphore()

    def greet(who):
        pl.semaphore_signal(barrier, inc=1, device_id=who, device_id_type=MESH)

    def plane_peer(o):
        return at((px + o[0]) % NX, (py + o[1]) % NY, pz, (core + o[2]) % 2)

    def z_peer(d):
        return at(px, py, (pz + d) % NZ, core)

    loads = [
        pltpu.make_async_copy(
            sales.at[:, pl.ds(i * CHUNK_ROWS, CHUNK_ROWS), :],
            x.at[:, pl.ds(i * CHUNK_ROWS, CHUNK_ROWS), :],
            load_sem.at[i],
        )
        for i in range(CHUNKS)
    ]
    smalls = [
        pltpu.make_async_copy(a, b, small_sem.at[i])
        for i, (a, b) in enumerate((
            (day_month, days_s), (product_category, cats_s), (store_region, regs_s),
            (month_year, years_s), (day_month, days_v), (product_category, cats_v),
            (store_region, regs_v), (month_year, years_v),
        ))
    ]
    for copy in smalls[:3]:
        copy.start()
    for copy in loads:
        copy.start()
    for copy in smalls[3:]:
        copy.start()

    for d in ZOFF:
        greet(z_peer(d))
    for o in PLANE:
        greet(plane_peer(o))
    for p in range(PROD):
        greet(((t + 1) % TM, p))
        greet(((t + TM - 1) % TM, p))

    for copy in smalls[:3]:
        copy.wait()

    lane = iota((8, 256), 1)
    key = jnp.zeros((8, 256), I32)
    for p in range(16):
        key = jnp.where(lane // 16 == p, cats_s[0, prod * 16 + p] * 4, key)
    reg = jnp.zeros((8, 256), I32)
    for s in range(16):
        reg = jnp.where(lane % 16 == s, regs_s[0, s], reg)
    key = key + reg
    hot = jnp.concatenate(
        [jnp.where(iota((8, 256), 0) + 8 * i == key, 1.0, 0.0) for i in range(16)], axis=0
    ).astype(BF16)

    row0 = t // 4
    lane0 = (t % 4) * DAYS
    masks = []
    for d in range(DAYS):
        month = days_s[row0, lane0 + d]
        other = t - 1 if d < DAYS // 2 else t + 1
        masks.append(jnp.full((8, 128), jnp.where(month == other, 1.0, 0.0), F32))

    def reduce_rows(i, carry):
        rows = pl.ds(pl.multiple_of(i * 8, 8), 8)
        mid = [jnp.zeros((8, 128), F32) for _ in range(2)]
        side = []
        for half in range(2):
            acc = jnp.zeros((8, 128), F32)
            for d in range(half * 16, half * 16 + 16):
                value = x[d, rows, :]
                kept = value * masks[d]
                acc = acc + kept
                mid[half] = mid[half] + (value - kept)
            side.append(acc)
        y[rows, 0:128] = side[0]
        y[rows, 128:256] = mid[0] + mid[1]
        y[rows, 256:384] = side[1]
        return carry

    sums = None
    for c in range(CHUNKS):
        loads[c].wait()
        lax.fori_loop(c * CHUNK_ROWS // 8, (c + 1) * CHUNK_ROWS // 8, reduce_rows, 0)
        if (c + 1) % (CHUNKS // 2) == 0:
            half = pl.ds(128 * (c // (CHUNKS // 2)), 128)
            for piece in split3(y[half, :]):
                more = jnp.dot(hot[:, half.start : half.start + 128], piece, preferred_element_type=F32)
                sums = more if sums is None else sums + more

    low = iota((8, 128), 0) < 4
    slots = [sums[:, 128 * k : 128 * k + 128] for k in range(3)]
    for k in range(3):
        part[k] = slots[k]
    for i in range(16):
        a, b, c = (slots[k][8 * i : 8 * i + 8] for k in range(3))
        pieces[2 * i, 0:8] = jnp.where(low, a, pltpu.roll(b, 4, 0))
        pieces[2 * i, 8:16] = c
        pieces[2 * i + 1, 0:8] = jnp.where(low, pltpu.roll(a, 4, 0), b)
        pieces[2 * i + 1, 8:16] = pltpu.roll(c, 4, 0)

    pl.semaphore_wait(barrier, len(ZOFF) + len(PLANE) + 2 * PROD)

    plane_copies = []
    for k, o in enumerate(PLANE):
        ax, ay, ac = (px + o[0]) % NX, (py + o[1]) % NY, (core + o[2]) % 2
        plane_copies.append(pltpu.make_async_remote_copy(
            src_ref=pieces.at[category_of(ax, ay, ac), pl.ds(0, 12), :],
            dst_ref=plane_in.at[k, pl.ds(0, 12), :],
            send_sem=plane_ss.at[k], recv_sem=plane_rs.at[k],
            device_id=at(ax, ay, pz, ac), device_id_type=MESH,
        ))
    for copy in plane_copies:
        copy.start()
    month_copies = []
    for n, (k, p) in enumerate(MONTH):
        to = (prod + p) % PROD
        month_copies.append(pltpu.make_async_remote_copy(
            src_ref=part.at[k, pl.ds(pl.multiple_of(to * 32, 32), 32), :],
            dst_ref=month_in.at[n],
            send_sem=month_ss.at[n], recv_sem=month_rs.at[n],
            device_id=((t + k - 1 + TM) % TM, to), device_id_type=MESH,
        ))

    for copy in smalls[3:]:
        copy.wait()
    months = iota((64, 128), 0)
    found = jnp.zeros((64, 128), F32)
    own_found = jnp.zeros((8, 128), F32)
    for i in range(16):
        line = days_v[i : i + 1, :]
        found = found + jnp.where(months == line, 1.0, 0.0)
    month_days = jnp.broadcast_to(jnp.sum(found, axis=1, keepdims=True), (64, 128))
    for i in range(2):
        own_found = own_found + jnp.where(days_v[8 * i : 8 * i + 8, :] == t, 1.0, 0.0)
    own_days = jnp.broadcast_to(
        jnp.sum(jnp.sum(own_found, axis=1, keepdims=True), axis=0, keepdims=True), (8, 128)
    )
    row32, lane64 = iota((32, 64), 0), iota((8, 64), 0)
    years_of = jnp.where(row32 // 4 == years_v[0:1, :], 1.0, 0.0).astype(BF16)
    year_days = jnp.dot(years_of, month_days.astype(BF16), preferred_element_type=F32)
    cats_of = cats_v[0:1, :]
    sizes = jnp.broadcast_to(
        jnp.sum(jnp.where(row32 == cats_of, 1.0, 0.0), axis=1, keepdims=True), (32, 128)
    )
    own_sizes = jnp.broadcast_to(
        jnp.sum(jnp.where(row32 // 4 + prod * 8 == cats_of, 1.0, 0.0), axis=1, keepdims=True),
        (32, 128),
    )
    own_sizes8 = jnp.broadcast_to(
        jnp.sum(jnp.where(lane64 + prod * 8 == cats_of, 1.0, 0.0), axis=1, keepdims=True),
        (8, 128),
    )
    regions = jnp.broadcast_to(
        jnp.sum(jnp.where(iota((32, 16), 0) % 4 == regs_v[0:1, :], 1.0, 0.0), axis=1, keepdims=True),
        (32, 128),
    )
    regions8 = regions[0:8]
    year_region_days = year_days * regions

    target = [jnp.where(low, 2 * i, 2 * i + 1) for i in range(4)]
    totals = [jnp.zeros((8, 128), F32) for _ in range(4)]

    def year_of(time, k):
        return years_s[0, jnp.clip(time + k - 1, 0, TM - 1)]

    gathered = {}
    for k, o in enumerate(PLANE):
        gathered.setdefault((o[0], o[1] % 2), []).append(k)
    for (dx, dy), ks in sorted(gathered.items(), key=lambda g: max(hops(*PLANE[k][:2]) for k in g[1])):
        if (dx, dy) == (0, 0):
            first, second = pieces[own_cat, 0:8], pieces[own_cat, 8:16]
        else:
            first = second = None
        for k in ks:
            plane_copies[k].wait_recv()
            one, two = plane_in[k, 0:8], plane_in[k, 8:16]
            first = one if first is None else first + one
            second = two if second is None else second + two
        time = ((py - dy + NY) % 2) * (NX * NZ) + pz * NX + (px - dx + NX) % NX
        year0, year1, year2 = (year_of(time, k) for k in range(3))
        swapped = pltpu.roll(first, 4, 0)
        second = jnp.where(low, second, pltpu.roll(second, 4, 0))
        straight_of = jnp.where(low, year0, year1)
        swapped_of = jnp.where(low, year1, year0)
        second_of = jnp.where(low, year2, year2)
        for i in range(4):
            totals[i] = totals[i] + (
                jnp.where(straight_of == target[i], first, 0.0)
                + jnp.where(swapped_of == target[i], swapped, 0.0)
                + jnp.where(second_of == target[i], second, 0.0)
            )
    for i in range(4):
        year_part[8 * i : 8 * i + 8, :] = totals[i]
    z_copies = [
        pltpu.make_async_remote_copy(
            src_ref=year_part, dst_ref=z_in.at[k], send_sem=z_ss.at[k], recv_sem=z_rs.at[k],
            device_id=z_peer(d), device_id_type=MESH,
        )
        for k, d in enumerate(ZOFF)
    ]
    for copy in z_copies:
        copy.start()
    for copy in month_copies:
        copy.start()

    for c in range(32):
        scale[32 * c : 32 * c + 32, :] = inv_root(
            jnp.maximum(year_region_days * jnp.broadcast_to(sizes[c : c + 1, :], (32, 128)), 1.0)
        )

    year = year_part[...]
    for k, copy in reversed(list(enumerate(z_copies))):
        copy.wait_recv()
        year = year + z_in[k]
    year_own[...] = year
    own_rows = cube.at[pl.ds(pl.multiple_of(own_cat * 32, 32), 32), :]
    ag_copies = []
    for k, (dx, dy) in enumerate(CHIPS):
        ag_copies.append(pltpu.make_async_remote_copy(
            src_ref=year_own, dst_ref=own_rows, send_sem=ag_ss.at[k], recv_sem=ag_rs.at[k],
            device_id=at((px + dx) % NX, (py + dy) % NY, pz, core), device_id_type=MESH,
        ))
    for copy in ag_copies:
        copy.start()
    core_copies = [pltpu.make_async_remote_copy(
        src_ref=year_own, dst_ref=own_rows, send_sem=core_ss.at[15], recv_sem=core_rs.at[15],
        device_id=sibling, device_id_type=MESH,
    )]
    core_copies[0].start()
    cube[pl.ds(pl.multiple_of(own_cat * 32, 32), 32), :] = year

    month = part[1, pl.ds(pl.multiple_of(prod * 32, 32), 32), :]
    for n, copy in enumerate(month_copies):
        copy.wait_recv()
        month = month + month_in[n]
    month_sum[...] = month
    own_reg = month[0:8] + month[8:16] + month[16:24] + month[24:32]
    own_reg = own_reg + pltpu.roll(own_reg, 4, 0)
    reg_out[...] = own_reg
    reg_copies = [
        pltpu.make_async_remote_copy(
            src_ref=reg_out, dst_ref=reg_in.at[p - 1],
            send_sem=reg_ss.at[p - 1], recv_sem=reg_rs.at[p - 1],
            device_id=(t, (prod + p) % PROD), device_id_type=MESH,
        )
        for p in range(1, PROD)
    ]
    for copy in reg_copies:
        copy.start()
    days32 = jnp.concatenate([own_days] * 4, axis=0)
    month_detail[...] = month * inv_root(jnp.maximum(days32 * own_sizes * regions, 1.0))
    by_cat = sum(month_sum[pl.ds(r, 8, stride=4), :] for r in range(4))
    month_category[...] = by_cat * inv_root(jnp.maximum(own_days * own_sizes8 * 16.0, 1.0))

    for k in reversed(range(len(CHIPS))):
        dx, dy = CHIPS[k]
        ag_copies[k].wait_recv()
        cat = category_of((px - dx + NX) % NX, (py - dy + NY) % NY, core)
        rows = cube.at[pl.ds(pl.multiple_of(cat * 32, 32), 32), :]
        copy = pltpu.make_async_remote_copy(
            src_ref=rows, dst_ref=rows, send_sem=core_ss.at[k], recv_sem=core_rs.at[k],
            device_id=sibling, device_id_type=MESH,
        )
        copy.start()
        core_copies.append(copy)
    region = own_reg
    for p, copy in enumerate(reg_copies):
        copy.wait_recv()
        region = region + reg_in[p]
    month_region[...] = region * inv_root(jnp.maximum(own_days * 64.0 * regions8, 1.0))
    total = jnp.sum(jnp.where(low, region, 0.0), axis=0, keepdims=True)
    month_totals[...] = jnp.broadcast_to(total, (8, 128)) * inv_root(own_days * 64.0 * 16.0)

    for copy in core_copies:
        copy.wait_recv()

    sums = jnp.zeros((32, 128), F32)
    for i in range(16):
        a = cube[64 * i : 64 * i + 32, :]
        b = cube[64 * i + 32 : 64 * i + 64, :]
        sums = sums + (a + b)
        a = a * scale[64 * i : 64 * i + 32, :]
        b = b * scale[64 * i + 32 : 64 * i + 64, :]
        for n in range(4):
            one, two = a[8 * n : 8 * n + 8], b[8 * n : 8 * n + 8]
            year_detail[(2 * n) * 128 + 8 * i : (2 * n) * 128 + 8 * i + 8, :] = jnp.where(
                low, one, pltpu.roll(two, 4, 0))
            year_detail[(2 * n + 1) * 128 + 8 * i : (2 * n + 1) * 128 + 8 * i + 8, :] = jnp.where(
                low, pltpu.roll(one, 4, 0), two)
    sums_v[...] = sums
    year_region[...] = sums * inv_root(jnp.maximum(year_region_days * 64.0, 1.0))
    for n in range(8):
        by_cat = sum(cube[pl.ds(4 * n + r, 32, stride=32), :] for r in range(4))
        days = jnp.broadcast_to(year_days[4 * n : 4 * n + 1, :], (32, 128))
        year_category[32 * n : 32 * n + 32, :] = by_cat * inv_root(
            jnp.maximum(days * sizes * 16.0, 1.0))
    days_of[...] = year_days
    days8 = days_of[pl.ds(0, 8, stride=4), :]
    total = sum(sums_v[pl.ds(r, 8, stride=4), :] for r in range(4))
    year_totals[...] = total * inv_root(days8 * 64.0 * 16.0)

    for copy in plane_copies + month_copies + z_copies + reg_copies + ag_copies + core_copies:
        copy.wait_send()


def finish(*refs):
    count = len(refs) // 2
    copies = [
        pltpu.make_async_copy(source.at[pl.ds(0, target.shape[0]), :], target, refs[-1].at[i])
        for i, (source, target) in enumerate(zip(refs[:count], refs[count:-1]))
    ]
    for copy in copies:
        copy.start()
    for copy in copies:
        copy.wait()


def shape(rows):
    return jax.ShapeDtypeStruct((rows, 128), F32)


def shards(sales_records, day_month, month_year, product_category, store_region):
    vmem = pl.BlockSpec(memory_space=pltpu.VMEM)
    anywhere = pl.BlockSpec(memory_space=pl.ANY)
    dma = pltpu.SemaphoreType.DMA
    found = pl.pallas_call(
        kernel,
        out_shape=[pltpu.VMEM((n, 128), F32) for n in (1024, 256, 32, 8, 32, 8, 8, 8)],
        in_specs=[anywhere] * 5,
        out_specs=[vmem] * 8,
        scratch_shapes=[
            pltpu.VMEM((16, 128), I32), pltpu.VMEM((1, 64), I32),
            pltpu.VMEM((1, 64), I32), pltpu.VMEM((1, 16), I32),
            pltpu.SMEM((16, 128), I32), pltpu.SMEM((1, 64), I32),
            pltpu.SMEM((1, 64), I32), pltpu.SMEM((1, 16), I32),
            pltpu.VMEM((32, 256, 128), F32),
            pltpu.VMEM((256, 384), F32),
            pltpu.VMEM((3, 128, 128), F32),
            pltpu.VMEM((32, 16, 128), F32),
            pltpu.VMEM((31, 16, 128), F32),
            pltpu.VMEM((32, 128), F32),
            pltpu.VMEM((7, 32, 128), F32),
            pltpu.VMEM((32, 128), F32),
            pltpu.VMEM((1024, 128), F32),
            pltpu.VMEM((11, 32, 128), F32),
            pltpu.VMEM((32, 128), F32),
            pltpu.VMEM((8, 128), F32),
            pltpu.VMEM((3, 8, 128), F32),
            pltpu.VMEM((1024, 128), F32),
            pltpu.VMEM((32, 128), F32),
            pltpu.VMEM((32, 128), F32),
            dma((8,)), dma((CHUNKS,)), dma((31,)), dma((31,)), dma((11,)), dma((11,)),
            dma((7,)), dma((7,)), dma((3,)), dma((3,)), dma((15,)), dma((15,)),
            dma((16,)), dma((16,)),
        ],
        compiler_params=pltpu.CompilerParams(collective_id=0, has_side_effects=True),
        name="cube",
    )(
        sales_records.reshape(32, 256, 128),
        day_month.reshape(16, 128),
        month_year.reshape(1, 64),
        product_category.reshape(1, 64),
        store_region.reshape(1, 16),
    )
    out = pl.pallas_call(
        finish,
        out_shape=[shape(n) for n in (1024, 256, 32, 8, 32, 8, 4, 1)],
        in_specs=[vmem] * 8,
        out_specs=[anywhere] * 8,
        scratch_shapes=[dma((8,))],
        name="finish",
    )(*(pltpu.with_memory_space_constraint(v, pltpu.VMEM) for v in found))
    yd, yc, yr, yt, md, mc, mr, mt = out
    return (
        md.reshape(1, 8, 4, 128), mc.reshape(1, 8, 128), mr.reshape(1, 4, 128), mt.reshape(1, 128),
        yd.reshape(8, 32, 4, 128), yc.reshape(8, 32, 128), yr.reshape(8, 4, 128), yt,
    )


def solution(mesh):
    placed = (P("tm", "prod", None, None), P(), P(), P(), P())
    return jax.shard_map(
        shards,
        mesh=mesh,
        in_specs=placed,
        out_specs=(
            P("tm", "prod", None, None), P("tm", "prod", None), P("tm", None, None), P("tm", None),
            P(), P(), P(), P(),
        ),
        check_vma=False,
    )
```

```python
import jax
import jax.numpy as jnp
from jax import lax
from jax.experimental import pallas as pl
from jax.experimental.pallas import tpu as pltpu
from jax.sharding import PartitionSpec as P

MESH = pl.DeviceIdType.MESH
F32 = jnp.float32
BF16 = jnp.bfloat16
I32 = jnp.int32

NX, NY, NZ = 4, 4, 8
TM, PROD = 64, 4
DAYS = 32
CHUNKS = 8
CHUNK_ROWS = 256 // CHUNKS


def hops(a, b):
    return min(a, 4 - a) + min(b, 4 - b)


PLANE = sorted(
    ((a, b, c) for a in range(4) for b in range(4) for c in range(2) if (a, b, c) != (0, 0, 0)),
    key=lambda o: -hops(o[0], o[1]),
)
CHIPS = [(a, b) for b in (2, 1, 3, 0) for a in (2, 1, 3, 0) if (a, b) != (0, 0)]
ZOFF = [4, 3, 5, 2, 6, 1, 7]
ROW_ORDER = (0, 1, 3, 2)
MONTH = [(k, p) for k in (0, 2, 1) for p in (2, 1, 3, 0) if (k, p) != (1, 0)]


def iota(shape, dim):
    return lax.broadcasted_iota(I32, shape, dim)


def split3(value):
    high = value.astype(BF16)
    rest = value - high.astype(F32)
    mid = rest.astype(BF16)
    low = (rest - mid.astype(F32)).astype(BF16)
    return high, mid, low


def inv_root(count):
    return 1.0 / jnp.sqrt(count)


def kernel(
    sales, day_month, month_year, product_category, store_region,
    year_detail, year_category, year_region, year_totals,
    month_detail, month_category, month_region, month_totals,
    days_v, years_v, cats_v, regs_v, days_s, years_s,
    x, y, part, pieces, plane_in, year_part, z_in, year_own, cube,
    month_in, month_sum, scale, cat_scale, sums_v, days_of,
    small_sem, load_sem, plane_ss, plane_rs, month_ss, month_rs, z_ss, z_rs,
    ag_ss, ag_rs, core_ss, core_rs,
):
    t, prod = lax.axis_index("tm"), lax.axis_index("prod")
    px, pz, ylo = t % NX, (t // NX) % NZ, t // (NX * NZ)
    core, yhi = prod % 2, prod // 2
    py = yhi * 2 + ylo

    def at(ax, ay, az, ac):
        return (ay % 2) * (NX * NZ) + az * NX + ax, (ay // 2) * 2 + ac

    def category_of(ax, ay, ac):
        return ((ay // 2) * 2 + ac) * 8 + (ay % 2) * NX + ax

    own_cat = category_of(px, py, core)
    sibling = (t, prod + 1 - 2 * core)

    def group(ref, send_sem, recv_sem):
        return pltpu.make_async_remote_copy(
            src_ref=ref, dst_ref=ref, send_sem=send_sem, recv_sem=recv_sem,
            device_id=sibling, device_id_type=MESH,
        )

    barrier = pltpu.get_barrier_semaphore()

    def greet(who):
        pl.semaphore_signal(barrier, inc=1, device_id=who, device_id_type=MESH)

    def plane_peer(o):
        return at((px + o[0]) % NX, (py + o[1]) % NY, pz, (core + o[2]) % 2)

    def z_peer(d):
        return at(px, py, (pz + d) % NZ, core)

    loads = [
        pltpu.make_async_copy(
            sales.at[:, pl.ds(i * CHUNK_ROWS, CHUNK_ROWS), :],
            x.at[:, pl.ds(i * CHUNK_ROWS, CHUNK_ROWS), :],
            load_sem.at[i],
        )
        for i in range(CHUNKS)
    ]
    smalls = [
        pltpu.make_async_copy(a, b, small_sem.at[i])
        for i, (a, b) in enumerate((
            (day_month, days_s), (product_category, cats_v), (store_region, regs_v),
            (month_year, years_s), (day_month, days_v), (month_year, years_v),
        ))
    ]
    for copy in smalls[:3]:
        copy.start()
    for copy in loads:
        copy.start()
    for copy in smalls[3:]:
        copy.start()

    for d in ZOFF:
        greet(z_peer(d))
    for o in PLANE:
        greet(plane_peer(o))
    for p in range(PROD):
        greet(((t + 1) % TM, p))
        greet(((t + TM - 1) % TM, p))

    for copy in smalls[:3]:
        copy.wait()

    pick_cat = jnp.where(iota((64, 256), 1) // 16 + prod * 16 == iota((64, 256), 0), 1.0, 0.0)
    pick_reg = jnp.where(iota((16, 256), 1) % 16 == iota((16, 256), 0), 1.0, 0.0)
    cat_row = jnp.broadcast_to(cats_v[0:1, :], (8, 64)).astype(F32) * 4.0
    reg_row = jnp.broadcast_to(regs_v[0:1, :], (8, 16)).astype(F32)
    key = (
        jnp.dot(cat_row.astype(BF16), pick_cat.astype(BF16), preferred_element_type=F32)
        + jnp.dot(reg_row.astype(BF16), pick_reg.astype(BF16), preferred_element_type=F32)
    ).astype(I32)
    hot = jnp.concatenate(
        [jnp.where(iota((8, 256), 0) + 8 * i == key, 1.0, 0.0) for i in range(16)], axis=0
    ).astype(BF16)

    row0 = t // 4
    lane0 = (t % 4) * DAYS
    masks = []
    for d in range(DAYS):
        month = days_s[row0, lane0 + d]
        other = t - 1 if d < DAYS // 2 else t + 1
        masks.append(jnp.full((8, 128), jnp.where(month == other, 1.0, 0.0), F32))

    def reduce_rows(i, carry):
        rows = pl.ds(pl.multiple_of(i * 8, 8), 8)
        mid = [jnp.zeros((8, 128), F32) for _ in range(2)]
        side = []
        for half in range(2):
            acc = jnp.zeros((8, 128), F32)
            for d in range(half * 16, half * 16 + 16):
                value = x[d, rows, :]
                kept = value * masks[d]
                acc = acc + kept
                mid[half] = mid[half] + (value - kept)
            side.append(acc)
        y[rows, 0:128] = side[0]
        y[rows, 128:256] = mid[0] + mid[1]
        y[rows, 256:384] = side[1]
        return carry

    sums = None
    for c in range(CHUNKS):
        loads[c].wait()
        lax.fori_loop(c * CHUNK_ROWS // 8, (c + 1) * CHUNK_ROWS // 8, reduce_rows, 0)
        if (c + 1) % (CHUNKS // 2) == 0:
            half = pl.ds(128 * (c // (CHUNKS // 2)), 128)
            for piece in split3(y[half, :]):
                more = jnp.dot(hot[:, half.start : half.start + 128], piece, preferred_element_type=F32)
                sums = more if sums is None else sums + more

    low = iota((8, 128), 0) < 4
    slots = [sums[:, 128 * k : 128 * k + 128] for k in range(3)]
    for i in range(16):
        a, b, c = (slots[k][8 * i : 8 * i + 8] for k in range(3))
        pieces[2 * i, 0:8] = jnp.where(low, a, pltpu.roll(b, 4, 0))
        pieces[2 * i, 8:16] = c
        pieces[2 * i + 1, 0:8] = jnp.where(low, pltpu.roll(a, 4, 0), b)
        pieces[2 * i + 1, 8:16] = pltpu.roll(c, 4, 0)

    pl.semaphore_wait(barrier, len(ZOFF) + len(PLANE) + 2 * PROD)

    plane_copies = []
    for k, o in enumerate(PLANE):
        ax, ay, ac = (px + o[0]) % NX, (py + o[1]) % NY, (core + o[2]) % 2
        plane_copies.append(pltpu.make_async_remote_copy(
            src_ref=pieces.at[category_of(ax, ay, ac), pl.ds(0, 12), :],
            dst_ref=plane_in.at[k, pl.ds(0, 12), :],
            send_sem=plane_ss, recv_sem=plane_rs,
            device_id=at(ax, ay, pz, ac), device_id_type=MESH,
        ))
    for copy in plane_copies:
        copy.start()

    for k in range(3):
        by_reg = sum(slots[k][8 * i : 8 * i + 8] for i in range(16))
        by_reg = by_reg + pltpu.roll(by_reg, 4, 0)
        for p in range(PROD):
            part[k, p, 0:32] = slots[k][32 * p : 32 * p + 32]
            part[k, p, 32:40] = by_reg
    month_copies = []
    for n, (k, p) in enumerate(MONTH):
        to = (prod + p) % PROD
        month_copies.append(pltpu.make_async_remote_copy(
            src_ref=part.at[k, to],
            dst_ref=month_in.at[n],
            send_sem=month_ss, recv_sem=month_rs,
            device_id=((t + k - 1 + TM) % TM, to), device_id_type=MESH,
        ))

    for copy in smalls[3:]:
        copy.wait()
    months = iota((64, 128), 0)
    found = jnp.zeros((64, 128), F32)
    own_found = jnp.zeros((8, 128), F32)
    for i in range(16):
        line = days_v[i : i + 1, :]
        found = found + jnp.where(months == line, 1.0, 0.0)
    month_days = jnp.broadcast_to(jnp.sum(found, axis=1, keepdims=True), (64, 128))
    for i in range(2):
        own_found = own_found + jnp.where(days_v[8 * i : 8 * i + 8, :] == t, 1.0, 0.0)
    own_days = jnp.broadcast_to(
        jnp.sum(jnp.sum(own_found, axis=1, keepdims=True), axis=0, keepdims=True), (8, 128)
    )
    row32, lane64 = iota((32, 64), 0), iota((8, 64), 0)
    years_of = jnp.where(row32 // 4 == years_v[0:1, :], 1.0, 0.0).astype(BF16)
    year_days = jnp.dot(years_of, month_days.astype(BF16), preferred_element_type=F32)
    cats_of = cats_v[0:1, :]
    sizes = jnp.broadcast_to(
        jnp.sum(jnp.where(row32 == cats_of, 1.0, 0.0), axis=1, keepdims=True), (32, 128)
    )
    own_sizes = jnp.broadcast_to(
        jnp.sum(jnp.where(row32 // 4 + prod * 8 == cats_of, 1.0, 0.0), axis=1, keepdims=True),
        (32, 128),
    )
    own_sizes8 = jnp.broadcast_to(
        jnp.sum(jnp.where(lane64 + prod * 8 == cats_of, 1.0, 0.0), axis=1, keepdims=True),
        (8, 128),
    )
    regions = jnp.broadcast_to(
        jnp.sum(jnp.where(iota((32, 16), 0) % 4 == regs_v[0:1, :], 1.0, 0.0), axis=1, keepdims=True),
        (32, 128),
    )
    regions8 = regions[0:8]
    year_region_days = year_days * regions

    target = [jnp.where(low, 2 * i, 2 * i + 1) for i in range(4)]
    totals = [jnp.zeros((8, 128), F32) for _ in range(4)]

    def year_of(time, k):
        return years_s[0, jnp.clip(time + k - 1, 0, TM - 1)]

    plane_group = group(plane_in.at[:, pl.ds(0, 12), :], plane_ss, plane_rs)
    plane_group.wait_recv()
    gathered = {}
    for k, o in enumerate(PLANE):
        gathered.setdefault((o[0], o[1] % 2), []).append(k)
    for (dx, dy), ks in sorted(gathered.items(), key=lambda g: max(hops(*PLANE[k][:2]) for k in g[1])):
        if (dx, dy) == (0, 0):
            first, second = pieces[own_cat, 0:8], pieces[own_cat, 8:16]
        else:
            first = second = None
        for k in ks:
            one, two = plane_in[k, 0:8], plane_in[k, 8:16]
            first = one if first is None else first + one
            second = two if second is None else second + two
        time = ((py - dy + NY) % 2) * (NX * NZ) + pz * NX + (px - dx + NX) % NX
        year0, year1, year2 = (year_of(time, k) for k in range(3))
        swapped = pltpu.roll(first, 4, 0)
        second = jnp.where(low, second, pltpu.roll(second, 4, 0))
        straight_of = jnp.where(low, year0, year1)
        swapped_of = jnp.where(low, year1, year0)
        second_of = jnp.where(low, year2, year2)
        for i in range(4):
            totals[i] = totals[i] + (
                jnp.where(straight_of == target[i], first, 0.0)
                + jnp.where(swapped_of == target[i], swapped, 0.0)
                + jnp.where(second_of == target[i], second, 0.0)
            )
    for i in range(4):
        year_part[8 * i : 8 * i + 8, :] = totals[i]
    z_copies = [
        pltpu.make_async_remote_copy(
            src_ref=year_part, dst_ref=z_in.at[k], send_sem=z_ss, recv_sem=z_rs,
            device_id=z_peer(d), device_id_type=MESH,
        )
        for k, d in enumerate(ZOFF)
    ]
    for copy in z_copies:
        copy.start()
    for copy in month_copies:
        copy.start()

    for c in range(32):
        scale[32 * c : 32 * c + 32, :] = inv_root(
            jnp.maximum(year_region_days * jnp.broadcast_to(sizes[c : c + 1, :], (32, 128)), 1.0)
        )

    def rows_of(cat, count):
        return pl.ds(pl.multiple_of(cat * 32, 32), count)

    for n in range(8):
        days = jnp.broadcast_to(year_days[4 * n : 4 * n + 1, :], (32, 128))
        cat_scale[32 * n : 32 * n + 32, :] = inv_root(jnp.maximum(days * sizes * 16.0, 1.0))
    reg_scale = inv_root(jnp.maximum(year_region_days * 64.0, 1.0))
    days_of[...] = year_days
    total_scale = inv_root(days_of[pl.ds(0, 8, stride=4), :] * 64.0 * 16.0)

    year = year_part[...]
    z_group = group(z_in, z_ss, z_rs)
    z_group.wait_recv()
    for k in range(len(ZOFF)):
        year = year + z_in[k]
    year_own[...] = year
    for dx, dy in CHIPS:
        pltpu.make_async_remote_copy(
            src_ref=year_own, dst_ref=cube.at[rows_of(own_cat, 32), :],
            send_sem=ag_ss, recv_sem=ag_rs.at[dy],
            device_id=at((px + dx) % NX, (py + dy) % NY, pz, core), device_id_type=MESH,
        ).start()
    cube[rows_of(own_cat, 32), :] = year

    month = part[1, prod]
    month_group = group(month_in, month_ss, month_rs)
    month_group.wait_recv()
    for n in range(len(MONTH)):
        month = month + month_in[n]
    region = month[32:40]
    month = month[0:32]
    month_sum[...] = month
    days32 = jnp.concatenate([own_days] * 4, axis=0)
    month_detail[...] = month * inv_root(jnp.maximum(days32 * own_sizes * regions, 1.0))
    by_cat = sum(month_sum[pl.ds(r, 8, stride=4), :] for r in range(4))
    month_category[...] = by_cat * inv_root(jnp.maximum(own_days * own_sizes8 * 16.0, 1.0))

    month_region[...] = region * inv_root(jnp.maximum(own_days * 64.0 * regions8, 1.0))
    total = jnp.sum(jnp.where(low, region, 0.0), axis=0, keepdims=True)
    month_totals[...] = jnp.broadcast_to(total, (8, 128)) * inv_root(own_days * 64.0 * 16.0)

    for dy in ROW_ORDER:
        group(cube.at[pl.ds(0, 128 if dy else 96), :], ag_ss, ag_rs.at[dy]).wait_recv()
        rows = cube.at[rows_of(category_of(0, (py - dy + NY) % NY, core), 128), :]
        pltpu.make_async_remote_copy(
            src_ref=rows, dst_ref=rows, send_sem=core_ss, recv_sem=core_rs,
            device_id=sibling, device_id_type=MESH,
        ).start()

    def finish_block(base, sums):
        for i in range(4):
            at_a, at_b = (
                pl.ds(pl.multiple_of((base + 2 * i + n) * 32, 32), 32) for n in range(2)
            )
            a, b = cube[at_a, :], cube[at_b, :]
            sums = sums + (a + b)
            a, b = a * scale[at_a, :], b * scale[at_b, :]
            for n in range(4):
                one, two = a[8 * n : 8 * n + 8], b[8 * n : 8 * n + 8]
                even = pl.ds(pl.multiple_of(256 * n + base * 4 + 8 * i, 8), 8)
                odd = pl.ds(pl.multiple_of(256 * n + 128 + base * 4 + 8 * i, 8), 8)
                year_detail[even, :] = jnp.where(low, one, pltpu.roll(two, 4, 0))
                year_detail[odd, :] = jnp.where(low, pltpu.roll(one, 4, 0), two)
        for n in range(8):
            by_cat = sum(cube[pl.ds(base * 32 + 4 * n + r, 8, stride=32), :] for r in range(4))
            rows = pl.ds(pl.multiple_of(32 * n + base, 8), 8)
            year_category[rows, :] = by_cat * cat_scale[rows, :]
        return sums

    sums = jnp.zeros((32, 128), F32)
    sums = finish_block(8 * core, sums)
    sums = finish_block(16 + 8 * core, sums)
    core_group = group(cube.at[pl.ds(0, 512), :], core_ss, core_rs)
    core_group.wait_recv()
    sums = finish_block(8 - 8 * core, sums)
    sums = finish_block(24 - 8 * core, sums)
    sums_v[...] = sums
    year_region[...] = sums * reg_scale
    total = sum(sums_v[pl.ds(r, 8, stride=4), :] for r in range(4))
    year_totals[...] = total * total_scale

    for done in (plane_group, month_group, z_group, core_group):
        done.wait_send()
    group(cube.at[pl.ds(0, 480), :], ag_ss, ag_rs.at[0]).wait_send()


def finish(*refs):
    count = len(refs) // 2
    copies = [
        pltpu.make_async_copy(source.at[pl.ds(0, target.shape[0]), :], target, refs[-1].at[i])
        for i, (source, target) in enumerate(zip(refs[:count], refs[count:-1]))
    ]
    for copy in copies:
        copy.start()
    for copy in copies:
        copy.wait()


def shape(rows):
    return jax.ShapeDtypeStruct((rows, 128), F32)


def shards(sales_records, day_month, month_year, product_category, store_region):
    vmem = pl.BlockSpec(memory_space=pltpu.VMEM)
    anywhere = pl.BlockSpec(memory_space=pl.ANY)
    dma = pltpu.SemaphoreType.DMA
    found = pl.pallas_call(
        kernel,
        out_shape=[pltpu.VMEM((n, 128), F32) for n in (1024, 256, 32, 8, 32, 8, 8, 8)],
        in_specs=[anywhere] * 5,
        out_specs=[vmem] * 8,
        scratch_shapes=[
            pltpu.VMEM((16, 128), I32), pltpu.VMEM((1, 64), I32),
            pltpu.VMEM((1, 64), I32), pltpu.VMEM((1, 16), I32),
            pltpu.SMEM((16, 128), I32), pltpu.SMEM((1, 64), I32),
            pltpu.VMEM((32, 256, 128), F32),
            pltpu.VMEM((256, 384), F32),
            pltpu.VMEM((3, 4, 40, 128), F32),
            pltpu.VMEM((32, 16, 128), F32),
            pltpu.VMEM((31, 16, 128), F32),
            pltpu.VMEM((32, 128), F32),
            pltpu.VMEM((7, 32, 128), F32),
            pltpu.VMEM((32, 128), F32),
            pltpu.VMEM((1024, 128), F32),
            pltpu.VMEM((11, 40, 128), F32),
            pltpu.VMEM((32, 128), F32),
            pltpu.VMEM((1024, 128), F32),
            pltpu.VMEM((256, 128), F32),
            pltpu.VMEM((32, 128), F32),
            pltpu.VMEM((32, 128), F32),
            dma((6,)), dma((CHUNKS,)), dma(()), dma(()), dma(()), dma(()),
            dma(()), dma(()), dma(()), dma((NY,)), dma(()), dma(()),
        ],
        compiler_params=pltpu.CompilerParams(collective_id=0, has_side_effects=True),
        name="cube",
    )(
        sales_records.reshape(32, 256, 128),
        day_month.reshape(16, 128),
        month_year.reshape(1, 64),
        product_category.reshape(1, 64),
        store_region.reshape(1, 16),
    )
    out = pl.pallas_call(
        finish,
        out_shape=[shape(n) for n in (1024, 256, 32, 8, 32, 8, 4, 1)],
        in_specs=[vmem] * 8,
        out_specs=[anywhere] * 8,
        scratch_shapes=[dma((8,))],
        name="finish",
    )(*(pltpu.with_memory_space_constraint(v, pltpu.VMEM) for v in found))
    yd, yc, yr, yt, md, mc, mr, mt = out
    return (
        md.reshape(1, 8, 4, 128), mc.reshape(1, 8, 128), mr.reshape(1, 4, 128), mt.reshape(1, 128),
        yd.reshape(8, 32, 4, 128), yc.reshape(8, 32, 128), yr.reshape(8, 4, 128), yt,
    )


def solution(mesh):
    placed = (P("tm", "prod", None, None), P(), P(), P(), P())
    return jax.shard_map(
        shards,
        mesh=mesh,
        in_specs=placed,
        out_specs=(
            P("tm", "prod", None, None), P("tm", "prod", None), P("tm", None, None), P("tm", None),
            P(), P(), P(), P(),
        ),
        check_vma=False,
    )
```
